128 devices in a mesh: kv: 64 (over z, x, y), head: 2 (over core).
Axes of the slice: x: 4, y: 4, z: 4, core: 2. Of those that a mesh axis runs over, the one named last changes fastest.
Arguments:
- queries: bfloat16 [8, 256, 128], P('head', 'kv'), may hold values from -384 to 384
- key_cache: bfloat16 [4096, 8, 128, 128], P('kv', 'head'), may hold values from -6 to 6
- value_cache: bfloat16 [4096, 8, 128, 128], P('kv', 'head'), may hold values from -6 to 6
- key_new: bfloat16 [32, 8, 128], P(None, 'head'), may hold values from -6 to 6
- value_new: bfloat16 [32, 8, 128], P(None, 'head'), may hold values from -6 to 6
- lengths: int32 [32], replicated, may hold values from 2 to 16385, as said below
- page_table: int32 [4096], replicated, may hold values from 0 to 4095, each once
Outputs:
- attended: bfloat16 [8, 256, 128], P('head', 'kv')
The draws below stay inside these ranges and needn't reach their ends.
Inputs may be any that keep to these rules, and one draw needn't show every extreme that they name: The cache holds the first lengths[s] - 1 tokens of sequence s; some sequence has the largest length. `page_table`: every page appears once; page g lies on kv index g // 64.
All inputs are finite; a program needn't handle non-finite values.
Results may differ from the reference program's by a relative error of at most 0.0025.
Values may be sent and summed in bfloat16 or wider, within the bound.
No kernel may reach another device: no remote copies, remote signals or barrier semaphores. Data moves between devices by JAX's collectives and lax.ppermute only.
A program may use at most 64 MiB of HBM per device.

```python
import math
import jax
import jax.numpy as jnp
from jax import lax

QH = 64
KVH = 8
HD = 128
PAGE = 128
MAXP = 128
SEQS = 32
PAGES = 4096


def draw_queries(key, part):
    normal_part = jax.random.normal(jax.random.fold_in(key, 11), (KVH, SEQS * (QH // KVH), HD), jnp.float32)
    values = jnp.clip(normal_part * 2.0, -8.0, 8.0)
    return values.astype(jnp.bfloat16)


def draw_lengths(key, part):
    most = MAXP * PAGE + 1
    values = jax.random.randint(jax.random.fold_in(key, 21), (SEQS,), 2, most + 1, jnp.int32)
    chosen = jax.random.randint(jax.random.fold_in(key, 22), (), 0, SEQS, jnp.int32)
    return jnp.where(jnp.arange(SEQS, dtype=jnp.int32) == chosen, most, values).astype(jnp.int32)


def block_levels(rng, shape, shards, low, largest):
    level, own = 1.0, jax.random.fold_in(rng, 6)
    for axis_at, shards_of in shards:
        draws = jnp.exp(jax.random.uniform(jax.random.fold_in(own, axis_at), (shards_of,), jnp.float32, low / len(shards), largest / len(shards)))
        level = level * jnp.repeat(draws, shape[axis_at] // shards_of).reshape([-1 if axis == axis_at else 1 for axis in range(len(shape))])
    return level


def noise(rng, dims, width, most, pieces=(), held_as=jnp.bfloat16):
    gain = block_levels(rng, dims, pieces, -0.22, 0.18) if pieces else 1.0
    entries = jax.random.normal(rng, dims, jnp.float32) * width * gain
    return jnp.minimum(jnp.maximum(entries, -most), most).astype(held_as)


def setup_inputs(seed: int = 0) -> dict:
    key_of = jax.random.split(jax.random.key(seed), 8)
    queries = draw_queries(jax.random.fold_in(key_of[7], 71), 0)
    key_cache = noise(key_of[1], (PAGES, KVH, PAGE, HD), 1.0, 6.0, ((0, 64), (1, 2)))
    value_cache = noise(key_of[2], (PAGES, KVH, PAGE, HD), 1.0, 6.0, ((0, 64), (1, 2)))
    key_new = noise(key_of[3], (SEQS, KVH, HD), 1.0, 6.0, ((1, 2),))
    value_new = noise(key_of[4], (SEQS, KVH, HD), 1.0, 6.0, ((1, 2),))
    lengths = draw_lengths(jax.random.fold_in(key_of[7], 71), 0)
    page_table = jax.random.permutation(key_of[6], PAGES).astype(jnp.int32)
    return {"queries": queries, "key_cache": key_cache, "value_cache": value_cache, "key_new": key_new, "value_new": value_new, "lengths": lengths, "page_table": page_table}


LOWEST_SCORE = -1e+30

def finish(cache_max, cache_sum, cache_out, query_wide, fresh_key, fresh_value, score_scale):
    new_score = lax.optimization_barrier(jnp.sum(query_wide * fresh_key.astype(jnp.float32), axis=-1)) * score_scale
    highest = jnp.maximum(cache_max, new_score)
    old_part = jnp.exp(cache_max - highest)
    new_part = jnp.exp(new_score - highest)
    numerator = cache_out * old_part[..., None] + new_part[..., None] * fresh_value.astype(jnp.float32)
    denominator = cache_sum * old_part + new_part
    return (numerator / denominator[..., None]).astype(jnp.bfloat16)

def reference(queries, key_cache, value_cache, key_new, value_new, lengths, page_table):
    seq_count = lengths.shape[0]
    kv_count = queries.shape[0]
    head_width = queries.shape[2]
    group_size = queries.shape[1] // seq_count
    page_total = key_cache.shape[0]
    page_len = key_cache.shape[2]
    page_slots = page_total // seq_count
    score_scale = 1.0 / math.sqrt(head_width)
    table = page_table.reshape(seq_count, page_slots).astype(jnp.int32)
    grouped = jnp.transpose(queries.reshape(kv_count, seq_count, group_size, head_width), (1, 0, 2, 3))
    offsets = jnp.arange(page_slots, dtype=jnp.int32)[:, None] * page_len + jnp.arange(page_len, dtype=jnp.int32)[None, :]

    def one_sequence(packed):
        query_rows, page_ids, length, fresh_key, fresh_value = packed
        keys = key_cache[page_ids].astype(jnp.float32)
        values = value_cache[page_ids].astype(jnp.float32)
        query_wide = query_rows.astype(jnp.float32)
        scores = jnp.einsum('gqd,mgtd->mgqt', query_wide, keys, precision=lax.Precision.HIGHEST) * score_scale
        in_cache = (offsets < length - 1)[:, None, None, :]
        masked = jnp.where(in_cache, scores, LOWEST_SCORE)
        page_max = lax.optimization_barrier(jnp.max(masked, axis=3))
        weights = jnp.where(in_cache, jnp.exp(masked - page_max[..., None]), 0.0)
        page_sum = lax.optimization_barrier(jnp.sum(weights, axis=3))
        rounded = lax.optimization_barrier(weights.astype(jnp.bfloat16)).astype(jnp.float32)
        page_out = jnp.einsum('mgqt,mgtd->mgqd', rounded, values, precision=lax.Precision.HIGHEST)
        cache_max = lax.optimization_barrier(jnp.max(page_max, axis=0))
        factor = jnp.exp(page_max - cache_max[None])
        cache_sum = lax.optimization_barrier(jnp.sum(page_sum * factor, axis=0))
        cache_out = lax.optimization_barrier(jnp.sum(page_out * factor[..., None], axis=0))
        return finish(cache_max, cache_sum, cache_out, query_wide, fresh_key[:, None, :], fresh_value[:, None, :], score_scale)
    result = lax.map(one_sequence, (grouped, table, lengths.astype(jnp.int32), key_new, value_new))
    return jnp.transpose(result, (1, 0, 2, 3)).reshape(kv_count, seq_count * group_size, head_width)
```

```python
import math

import jax
import jax.numpy as jnp
from jax import lax
from jax.experimental import pallas as pl
from jax.experimental.pallas import tpu as pltpu
from jax.sharding import PartitionSpec as P

LOWEST = -1e30
GROUP = 8
MIB = 1024 * 1024


def attend_kernel(
    scale2, plan_ref, arrived_ref, k_hbm, v_hbm, send_ref,
    k_ref, v_ref, q_ref, score_ref, prob_ref, pmax_ref, max_ref, sum_ref, out_ref, k_sem, v_sem,
):
    pages = k_ref.shape[0]
    seqs, pairs = q_ref.shape[0], q_ref.shape[1]
    token = lax.broadcasted_iota(jnp.int32, (8, 128), 1)
    upper = lax.broadcasted_iota(jnp.int32, (8, 128), 0) < 4
    groups = plan_ref[pages]

    def page_of(i):
        return plan_ref[i] & (pages - 1)

    def seq_of(i):
        return (plan_ref[i] // pages) & (seqs - 1)

    def copy(hbm, vmem, sem, i):
        return pltpu.make_async_copy(hbm.at[page_of(i)], vmem.at[i], sem.at[i])

    def start(hbm, vmem, sem):
        def some(g, _):
            for u in range(GROUP):
                copy(hbm, vmem, sem, g * GROUP + u).start()
            return 0

        lax.fori_loop(0, groups, some, 0)

    start(k_hbm, k_ref, k_sem)
    start(v_hbm, v_ref, v_sem)

    max_ref[...] = jnp.full(max_ref.shape, LOWEST, jnp.float32)
    sum_ref[...] = jnp.zeros(sum_ref.shape, jnp.float32)
    out_ref[...] = jnp.zeros(out_ref.shape, jnp.float32)

    def regroup(s, _):
        for h in range(2):
            for j in range(pairs):
                q_ref[s, j, 8 * h : 8 * h + 8] = arrived_ref[2 * s + h, 8 * j : 8 * j + 8]
        return 0

    lax.fori_loop(0, seqs, regroup, 0, unroll=4)

    def each(g, body):
        for u in range(GROUP):
            body(g * GROUP + u)

    def wait_for(hbm, vmem, sem, g):
        each(g, lambda i: copy(hbm, vmem, sem, i).wait())

    def score(i):
        s = seq_of(i)
        for j in range(pairs):
            keys = k_ref[i, 2 * j : 2 * j + 2].reshape(256, 128)
            both = lax.dot_general(
                q_ref[s, j], keys, (((1,), (1,)), ((), ())), preferred_element_type=jnp.float32
            )
            for h in range(2):
                rows = slice(8 * h, 8 * h + 8)
                score_ref[i, j, h] = jnp.where(upper, both[rows, :128], both[rows, 128:])

    def weigh(i):
        s = seq_of(i)
        inside = token < plan_ref[i] // (pages * seqs)
        for j in range(pairs):
            for h in range(2):
                score = jnp.where(inside, score_ref[i, j, h], LOWEST)
                top = jnp.max(score, axis=1, keepdims=True)
                prob_ref[i, j, h] = jnp.where(inside, jnp.exp2((score - top) * scale2), 0.0)
                top = jnp.broadcast_to(top, (8, 128))
                pmax_ref[i, j, h] = top
                max_ref[s, j, h] = jnp.maximum(max_ref[s, j, h], top)

    def combine(i):
        for j in range(pairs):
            probs = jnp.concatenate([prob_ref[i, j, 0], prob_ref[i, j, 1]], axis=0)
            values = jnp.concatenate([v_ref[i, 2 * j], v_ref[i, 2 * j + 1]], axis=1)
            both = jnp.dot(probs.astype(jnp.bfloat16), values, preferred_element_type=jnp.float32)
            for h in range(2):
                rows = slice(8 * h, 8 * h + 8)
                score_ref[i, j, h] = jnp.where(upper, both[rows, :128], both[rows, 128:])

    def gather(i):
        s = seq_of(i)
        for j in range(pairs):
            for h in range(2):
                factor = jnp.exp2((pmax_ref[i, j, h] - max_ref[s, j, h]) * scale2)
                sum_ref[s, j, h] = sum_ref[s, j, h] + factor * prob_ref[i, j, h]
                out_ref[s, j, h] = out_ref[s, j, h] + factor * score_ref[i, j, h]

    def staged(hbm, vmem, sem, first, second):
        wait_for(hbm, vmem, sem, 0)
        each(0, first)

        def step(g, _):
            wait_for(hbm, vmem, sem, g)
            each(g - 1, second)
            each(g, first)
            return 0

        lax.fori_loop(1, groups, step, 0)
        each(groups - 1, second)

    staged(k_hbm, k_ref, k_sem, score, weigh)
    staged(v_hbm, v_ref, v_sem, combine, gather)

    def pack(s, _):
        for h in range(2):
            note = jnp.zeros((8, 128), jnp.float32)
            for j in range(pairs):
                send_ref[2 * s + h, 8 * j : 8 * j + 8] = out_ref[s, j, h]
                total = jnp.sum(sum_ref[s, j, h], axis=1, keepdims=True)
                note = jnp.where(token == j, max_ref[s, j, h], note)
                note = jnp.where(token == pairs + j, total, note)
            send_ref[2 * s + h, 8 * pairs :] = note
        return 0

    lax.fori_loop(0, seqs, pack, 0, unroll=4)


def merge_kernel(scale2, seq_ref, recv_ref, q_ref, k_ref, v_ref, o_ref):
    sources = recv_ref.shape[0]
    pairs = q_ref.shape[0] // 8
    lane = lax.broadcasted_iota(jnp.int32, (8, 128), 1)
    upper = lax.broadcasted_iota(jnp.int32, (8, 128), 0) < 4
    s = seq_ref[0]
    keys = k_ref[s].astype(jnp.float32)
    fresh = v_ref[s].astype(jnp.float32)
    query = q_ref[...].astype(jnp.float32)

    def spread(x, j):
        low = jnp.broadcast_to(x[2 * j : 2 * j + 1], (8, 128))
        high = jnp.broadcast_to(x[2 * j + 1 : 2 * j + 2], (8, 128))
        return jnp.where(upper, low, high)

    new = jnp.full((8, 128), LOWEST, jnp.float32)
    for j in range(pairs):
        score = jnp.sum(query[8 * j : 8 * j + 8] * spread(keys, j), axis=1, keepdims=True)
        new = jnp.where(lane == j, score, new)
    top = new
    for d in range(sources):
        top = jnp.maximum(top, recv_ref[d, 8 * pairs :])
    top = jnp.where(lane < pairs, top, 0.0)
    fresh_weight = jnp.where(lane < pairs, jnp.exp2((new - top) * scale2), 0.0)
    totals = [jnp.zeros((8, 128), jnp.float32) for _ in range(pairs)]
    outs = []
    weights = [jnp.broadcast_to(fresh_weight[:, j : j + 1], (8, 128)) for j in range(pairs)]
    for j in range(pairs):
        outs.append(weights[j] * spread(fresh, j))
    for d in range(sources):
        note = recv_ref[d, 8 * pairs :]
        weight = jnp.exp2(jnp.where(lane < pairs, note - top, 0.0) * scale2)
        for j in range(pairs):
            w = jnp.broadcast_to(weight[:, j : j + 1], (8, 128))
            totals[j] = totals[j] + w * note
            outs[j] = outs[j] + w * recv_ref[d, 8 * j : 8 * j + 8]
    for j in range(pairs):
        at = pairs + j
        total = totals[j][:, at : at + 1] + weights[j][:, at : at + 1]
        done = (outs[j] / total).astype(o_ref.dtype)
        o_ref[2 * j] = done[:4]
        o_ref[2 * j + 1] = done[4:]


def plan_pages(kv_index, pages, page_len, lengths, page_table):
    seqs = lengths.shape[0]
    total = page_table.shape[0]
    slots = total // seqs
    here = jnp.arange(pages, dtype=jnp.int32)
    hit = page_table[None, :] == (kv_index * pages + here)[:, None]
    place = jnp.sum(jnp.where(hit, jnp.arange(total, dtype=jnp.int32)[None, :], 0), axis=1)
    seq, slot = place // slots, place % slots
    owner = seq[:, None] == jnp.arange(seqs, dtype=jnp.int32)[None, :]
    length = jnp.sum(jnp.where(owner, lengths[None, :], 0), axis=1)
    inside = jnp.clip(length - 1 - slot * page_len, 0, page_len)
    used = inside > 0
    code = here + pages * (seq + seqs * inside)
    rank = jnp.sum(jnp.where(used[None, :] & (here[None, :] < here[:, None]), 1, 0), axis=1)
    put = used[None, :] & (rank[None, :] == here[:, None])
    order = jnp.sum(jnp.where(put, code[None, :], 0), axis=1)
    count = jnp.sum(jnp.where(used, 1, 0))
    groups = jnp.maximum((count + GROUP - 1) // GROUP, 1)
    return jnp.concatenate([order, jnp.broadcast_to(groups, (pages,))])


def on_device(queries, key_cache, value_cache, key_new, value_new, lengths, page_table):
    kv_here, local_rows, head_width = queries.shape
    pages_here = key_cache.shape[0]
    page_len = key_cache.shape[2]
    seq_count = lengths.shape[0]
    devices = lax.axis_size("kv")
    pairs = kv_here // 2
    rows = kv_here * local_rows
    scale2 = math.log2(math.e) / math.sqrt(head_width)
    kv_index = lax.axis_index("kv")

    mine = queries.reshape(rows, head_width)
    arrived = lax.all_to_all(
        jnp.broadcast_to(mine[None], (devices, rows, head_width)), "kv", 0, 0, tiled=True
    )
    plan = plan_pages(kv_index, pages_here, page_len, lengths, page_table)

    vmem = pl.BlockSpec(memory_space=pltpu.VMEM)
    smem = pl.BlockSpec(memory_space=pltpu.SMEM)
    hbm = pl.BlockSpec(memory_space=pltpu.HBM)
    by_page = pltpu.VMEM((pages_here, pairs, 2, 8, 128), jnp.float32)
    by_seq = pltpu.VMEM((seq_count, pairs, 2, 8, 128), jnp.float32)
    cached = pltpu.VMEM(key_cache.shape, jnp.bfloat16)
    sent = pl.pallas_call(
        lambda *refs: attend_kernel(scale2, *refs),
        out_shape=jax.ShapeDtypeStruct((devices, rows + 8, head_width), jnp.float32),
        in_specs=[smem, vmem, hbm, hbm],
        out_specs=vmem,
        scratch_shapes=[
            cached,
            cached,
            pltpu.VMEM((seq_count, pairs, 16, head_width), jnp.bfloat16),
            by_page,
            by_page,
            by_page,
            by_seq,
            by_seq,
            by_seq,
            pltpu.SemaphoreType.DMA((pages_here,)),
            pltpu.SemaphoreType.DMA((pages_here,)),
        ],
        name="attend",
        compiler_params=pltpu.CompilerParams(vmem_limit_bytes=52 * MIB),
    )(plan, arrived, key_cache, value_cache)

    received = lax.all_to_all(sent, "kv", 0, 0, tiled=True)

    return pl.pallas_call(
        lambda *refs: merge_kernel(scale2, *refs),
        out_shape=jax.ShapeDtypeStruct(queries.shape, jnp.bfloat16),
        in_specs=[smem, vmem, vmem, vmem, vmem],
        out_specs=vmem,
        name="merge",
        compiler_params=pltpu.CompilerParams(vmem_limit_bytes=8 * MIB),
    )((kv_index // 2).reshape(1).astype(jnp.int32), received, mine, key_new, value_new)


def solution(mesh):
    placed = (
        P("head", "kv", None),
        P("kv", "head", None, None),
        P("kv", "head", None, None),
        P(None, "head", None),
        P(None, "head", None),
        P(),
        P(),
    )
    return jax.shard_map(
        on_device, mesh=mesh, in_specs=placed, out_specs=P("head", "kv", None), check_vma=False
    )
```

```python
import math

import jax
import jax.numpy as jnp
from jax import lax
from jax.experimental import pallas as pl
from jax.experimental.pallas import tpu as pltpu
from jax.sharding import PartitionSpec as P

LOWEST = -1e30
GROUP = 8
FIRST = 42
MIB = 1024 * 1024


def attend_kernel(
    scale2, plan_ref, arrived_ref, k_hbm, v_hbm, send_ref,
    k_ref, v_ref, q_ref, score_ref, prob_ref, pmax_ref, max_ref, sum_ref, out_ref, k_sem, v_sem,
):
    pages = k_ref.shape[0]
    seqs, pairs = q_ref.shape[0], q_ref.shape[1]
    token = lax.broadcasted_iota(jnp.int32, (8, 128), 1)
    upper = lax.broadcasted_iota(jnp.int32, (8, 128), 0) < 4
    groups = plan_ref[pages]

    def page_of(i):
        return plan_ref[i] & (pages - 1)

    def seq_of(i):
        return (plan_ref[i] // pages) & (seqs - 1)

    def copy(hbm, vmem, sem, g, u):
        i = g * GROUP + u
        return pltpu.make_async_copy(hbm.at[page_of(i)], vmem.at[i], sem.at[g])

    def start(hbm, vmem, sem):
        def some(g, _):
            for u in range(GROUP):
                copy(hbm, vmem, sem, g, u).start()
            return 0

        lax.fori_loop(0, groups, some, 0)

    start(k_hbm, k_ref, k_sem)
    start(v_hbm, v_ref, v_sem)

    max_ref[...] = jnp.full(max_ref.shape, LOWEST, jnp.float32)
    sum_ref[...] = jnp.zeros(sum_ref.shape, jnp.float32)
    out_ref[...] = jnp.zeros(out_ref.shape, jnp.float32)

    def regroup(s, _):
        for h in range(2):
            for j in range(pairs):
                q_ref[s, j, 8 * h : 8 * h + 8] = arrived_ref[(2 * s + h - FIRST) % (2 * seqs), 8 * j : 8 * j + 8]
        return 0

    lax.fori_loop(0, seqs, regroup, 0, unroll=4)

    def each(g, body):
        for u in range(GROUP):
            body(g * GROUP + u)

    def wait_for(hbm, vmem, sem, g):
        part = pl.ds(g * GROUP, GROUP)
        pltpu.make_async_copy(hbm.at[pl.ds(0, GROUP)], vmem.at[part], sem.at[g]).wait()

    def score(i):
        s = seq_of(i)
        for j in range(pairs):
            keys = k_ref[i, 2 * j : 2 * j + 2].reshape(256, 128)
            both = lax.dot_general(
                q_ref[s, j], keys, (((1,), (1,)), ((), ())), preferred_element_type=jnp.float32
            )
            for h in range(2):
                rows = slice(8 * h, 8 * h + 8)
                score_ref[i, j, h] = jnp.where(upper, both[rows, :128], both[rows, 128:])

    def weigh(i):
        s = seq_of(i)
        inside = token < plan_ref[i] // (pages * seqs)
        for j in range(pairs):
            for h in range(2):
                score = jnp.where(inside, score_ref[i, j, h], LOWEST)
                top = jnp.max(score, axis=1, keepdims=True)
                prob_ref[i, j, h] = jnp.where(inside, jnp.exp2((score - top) * scale2), 0.0)
                top = jnp.broadcast_to(top, (8, 128))
                pmax_ref[i, j, h] = top
                max_ref[s, j, h] = jnp.maximum(max_ref[s, j, h], top)

    def combine(i):
        for j in range(pairs):
            probs = jnp.concatenate([prob_ref[i, j, 0], prob_ref[i, j, 1]], axis=0)
            values = jnp.concatenate([v_ref[i, 2 * j], v_ref[i, 2 * j + 1]], axis=1)
            both = jnp.dot(probs.astype(jnp.bfloat16), values, preferred_element_type=jnp.float32)
            for h in range(2):
                rows = slice(8 * h, 8 * h + 8)
                score_ref[i, j, h] = jnp.where(upper, both[rows, :128], both[rows, 128:])

    def gather(i):
        s = seq_of(i)
        for j in range(pairs):
            for h in range(2):
                factor = jnp.exp2((pmax_ref[i, j, h] - max_ref[s, j, h]) * scale2)
                sum_ref[s, j, h] = sum_ref[s, j, h] + factor * prob_ref[i, j, h]
                out_ref[s, j, h] = out_ref[s, j, h] + factor * score_ref[i, j, h]

    def staged(hbm, vmem, sem, first, second):
        wait_for(hbm, vmem, sem, 0)
        each(0, first)

        def step(g, _):
            wait_for(hbm, vmem, sem, g)
            each(g - 1, second)
            each(g, first)
            return 0

        lax.fori_loop(1, groups, step, 0)
        each(groups - 1, second)

    staged(k_hbm, k_ref, k_sem, score, weigh)
    staged(v_hbm, v_ref, v_sem, combine, gather)

    kind = token % 4
    left = token < 4

    def pack(s, _):
        for h in range(2):
            to = (2 * s + h - FIRST) % (2 * seqs)
            note = jnp.zeros((8, 128), jnp.float32)
            for j in range(pairs):
                send_ref[to, 2 * j] = out_ref[s, j, h][:4]
                send_ref[to, 2 * j + 1] = out_ref[s, j, h][4:]
                total = jnp.sum(sum_ref[s, j, h], axis=1, keepdims=True)
                note = jnp.where(kind == j, max_ref[s, j, h], note)
                note = jnp.where(kind == pairs + j, total, note)
            send_ref[to, 2 * pairs] = jnp.where(left, note, pltpu.roll(note, 4, 0))[:4]
        return 0

    lax.fori_loop(0, seqs, pack, 0, unroll=4)


def attend(plan, arrived, key_cache, value_cache):
    pages_here, kv_here, page_len, head_width = key_cache.shape
    devices, rows, _ = arrived.shape
    seq_count, pairs = devices // 2, kv_here // 2
    scale2 = math.log2(math.e) / math.sqrt(head_width)
    vmem = pl.BlockSpec(memory_space=pltpu.VMEM)
    smem = pl.BlockSpec(memory_space=pltpu.SMEM)
    hbm = pl.BlockSpec(memory_space=pltpu.HBM)
    by_page = pltpu.VMEM((pages_here, pairs, 2, 8, 128), jnp.float32)
    by_seq = pltpu.VMEM((seq_count, pairs, 2, 8, 128), jnp.float32)
    cached = pltpu.VMEM(key_cache.shape, jnp.bfloat16)
    return pl.pallas_call(
        lambda *refs: attend_kernel(scale2, *refs),
        out_shape=jax.ShapeDtypeStruct((devices, kv_here + 1, rows // kv_here, head_width), jnp.float32),
        in_specs=[smem, vmem, hbm, hbm],
        out_specs=vmem,
        scratch_shapes=[
            cached,
            cached,
            pltpu.VMEM((seq_count, pairs, 16, head_width), jnp.bfloat16),
            by_page,
            by_page,
            by_page,
            by_seq,
            by_seq,
            by_seq,
            pltpu.SemaphoreType.DMA((pages_here // GROUP,)),
            pltpu.SemaphoreType.DMA((pages_here // GROUP,)),
        ],
        name="attend",
        compiler_params=pltpu.CompilerParams(vmem_limit_bytes=52 * MIB),
    )(plan, arrived, key_cache, value_cache)


def merge_kernel(scale2, recv_ref, q_ref, k_ref, v_ref, o_ref, note_ref):
    sources = recv_ref.shape[0]
    pairs = q_ref.shape[0] // 8
    notes = 2 * pairs
    lane = lax.broadcasted_iota(jnp.int32, (8, 128), 1)
    upper = lax.broadcasted_iota(jnp.int32, (8, 128), 0) < 4
    keys = k_ref[...].astype(jnp.float32)
    fresh = v_ref[...].astype(jnp.float32)
    query = q_ref[...].astype(jnp.float32)

    def spread(x, j):
        low = jnp.broadcast_to(x[2 * j : 2 * j + 1], (8, 128))
        high = jnp.broadcast_to(x[2 * j + 1 : 2 * j + 2], (8, 128))
        return jnp.where(upper, low, high)

    new = jnp.full((8, 128), LOWEST, jnp.float32)
    for j in range(pairs):
        score = jnp.sum(query[8 * j : 8 * j + 8] * spread(keys, j), axis=1, keepdims=True)
        new = jnp.where(lane == j, score, new)
    top = new
    for d in range(sources):
        part = recv_ref[d, 2 * pairs]
        note = jnp.concatenate([part, pltpu.roll(part, 128 - notes, 1)], axis=0)
        note_ref[d] = note
        top = jnp.maximum(top, note)
    top = jnp.where(lane < pairs, top, 0.0)
    fresh_weight = jnp.where(lane < pairs, jnp.exp2((new - top) * scale2), 0.0)
    totals = [jnp.zeros((8, 128), jnp.float32) for _ in range(pairs)]
    outs = []
    weights = [jnp.broadcast_to(fresh_weight[:, j : j + 1], (8, 128)) for j in range(pairs)]
    for j in range(pairs):
        outs.append(weights[j] * spread(fresh, j))
    for d in range(sources):
        note = note_ref[d]
        weight = jnp.exp2(jnp.where(lane < pairs, note - top, 0.0) * scale2)
        for j in range(pairs):
            w = jnp.broadcast_to(weight[:, j : j + 1], (8, 128))
            totals[j] = totals[j] + w * note
            part = jnp.concatenate([recv_ref[d, 2 * j], recv_ref[d, 2 * j + 1]], axis=0)
            outs[j] = outs[j] + w * part
    for j in range(pairs):
        at = pairs + j
        total = totals[j][:, at : at + 1] + weights[j][:, at - pairs : at - pairs + 1]
        done = (outs[j] / total).astype(o_ref.dtype)
        o_ref[2 * j] = done[:4]
        o_ref[2 * j + 1] = done[4:]


def plan_pages(kv_index, pages, page_len, lengths, page_table):
    seqs = lengths.shape[0]
    total = page_table.shape[0]
    slots = total // seqs
    here = jnp.arange(pages, dtype=jnp.int32)
    hit = page_table[None, :] == (kv_index * pages + here)[:, None]
    place = jnp.sum(jnp.where(hit, jnp.arange(total, dtype=jnp.int32)[None, :], 0), axis=1)
    seq, slot = place // slots, place % slots
    owner = seq[:, None] == jnp.arange(seqs, dtype=jnp.int32)[None, :]
    length = jnp.sum(jnp.where(owner, lengths[None, :], 0), axis=1)
    inside = jnp.clip(length - 1 - slot * page_len, 0, page_len)
    used = inside > 0
    code = here + pages * (seq + seqs * inside)
    rank = jnp.sum(jnp.where(used[None, :] & (here[None, :] < here[:, None]), 1, 0), axis=1)
    put = used[None, :] & (rank[None, :] == here[:, None])
    order = jnp.sum(jnp.where(put, code[None, :], 0), axis=1)
    count = jnp.sum(jnp.where(used, 1, 0))
    groups = jnp.maximum((count + GROUP - 1) // GROUP, 1)
    return jnp.concatenate([order, jnp.broadcast_to(groups, (pages,))])


def exchange(x):
    devices = x.shape[0]
    order = [(d + FIRST) % devices for d in range(devices)]
    return lax.all_to_all(x, "kv", 0, 0, tiled=True, axis_index_groups=[order])


def on_device(queries, key_cache, value_cache, key_new, value_new, lengths, page_table):
    kv_here, local_rows, head_width = queries.shape
    pages_here = key_cache.shape[0]
    page_len = key_cache.shape[2]
    seq_count = lengths.shape[0]
    devices = lax.axis_size("kv")
    pairs = kv_here // 2
    rows = kv_here * local_rows
    scale2 = math.log2(math.e) / math.sqrt(head_width)
    kv_index = lax.axis_index("kv")

    mine = queries.reshape(rows, head_width)
    arrived = exchange(jnp.broadcast_to(mine[None], (devices, rows, head_width)))
    plan = plan_pages(kv_index, pages_here, page_len, lengths, page_table)
    own = kv_index * local_rows // (devices * local_rows // seq_count)
    fresh_key = lax.dynamic_index_in_dim(key_new, own, 0, keepdims=False)
    fresh_value = lax.dynamic_index_in_dim(value_new, own, 0, keepdims=False)
    plan, fresh_key, fresh_value = lax.optimization_barrier((plan, fresh_key, fresh_value))

    sent = attend(plan, arrived, key_cache, value_cache)

    vmem = pl.BlockSpec(memory_space=pltpu.VMEM)
    received = exchange(sent)

    return pl.pallas_call(
        lambda *refs: merge_kernel(scale2, *refs),
        out_shape=jax.ShapeDtypeStruct(queries.shape, jnp.bfloat16),
        in_specs=[vmem] * 4,
        out_specs=vmem,
        scratch_shapes=[pltpu.VMEM((devices, 8, head_width), jnp.float32)],
        name="merge",
        compiler_params=pltpu.CompilerParams(vmem_limit_bytes=8 * MIB),
    )(received, mine, fresh_key, fresh_value)


def solution(mesh):
    placed = (
        P("head", "kv", None),
        P("kv", "head", None, None),
        P("kv", "head", None, None),
        P(None, "head", None),
        P(None, "head", None),
        P(),
        P(),
    )
    return jax.shard_map(
        on_device, mesh=mesh, in_specs=placed, out_specs=P("head", "kv", None), check_vma=False
    )
```

```python
import math

import jax
import jax.numpy as jnp
from jax import lax
from jax.experimental import pallas as pl
from jax.experimental.pallas import tpu as pltpu
from jax.sharding import PartitionSpec as P

LOWEST = -1e30
SCORE_UNIT = 1.0 / 8.0
NO_SCORE = -480000.0
MOST_POWER = 120.0
GROUP = 8
QUERY_FIRST = 42
RESULT_FIRST = 42
MIB = 1024 * 1024


def attend_kernel(
    scale2, plan_ref, arrived_ref, k_hbm, v_hbm, send_ref,
    list_ref, k_ref, v_ref, q_ref, score_ref, prob_ref, pmax_ref, max_ref, sum_ref, out_ref, k_sem, v_sem,
):
    pages = k_ref.shape[0]
    seqs, pairs = q_ref.shape[0], q_ref.shape[1]
    token = lax.broadcasted_iota(jnp.int32, (8, 128), 1)
    upper = lax.broadcasted_iota(jnp.int32, (8, 128), 0) < 4

    def page_of(i):
        return list_ref[i] & (pages - 1)

    def seq_of(i):
        return (list_ref[i] // pages) & (seqs - 1)

    def start(hbm, vmem, sem, i):
        pltpu.make_async_copy(hbm.at[page_of(i)], vmem.at[i], sem.at[i // GROUP]).start()

    def find(p, count):
        code = plan_ref[0, p]
        used = code >= seqs
        list_ref[count] = code * pages + p

        @pl.when(used)
        def _():
            start(k_hbm, k_ref, k_sem, count)

        return count + used.astype(jnp.int32)

    count = lax.fori_loop(0, pages, find, 0, unroll=4)
    groups = jnp.maximum((count + GROUP - 1) // GROUP, 1)

    def pad(i, _):
        list_ref[i] = 0
        start(k_hbm, k_ref, k_sem, i)
        return 0

    lax.fori_loop(count, groups * GROUP, pad, 0)

    def rest(g, _):
        for u in range(GROUP):
            start(v_hbm, v_ref, v_sem, g * GROUP + u)
        return 0

    lax.fori_loop(0, groups, rest, 0)

    max_ref[...] = jnp.full(max_ref.shape, LOWEST, jnp.float32)
    sum_ref[...] = jnp.zeros(sum_ref.shape, jnp.float32)
    out_ref[...] = jnp.zeros(out_ref.shape, jnp.float32)

    def regroup(s, _):
        for h in range(2):
            for j in range(pairs):
                q_ref[s, j, 8 * h : 8 * h + 8] = arrived_ref[(2 * s + h - QUERY_FIRST) % (2 * seqs), 8 * j : 8 * j + 8]
        return 0

    lax.fori_loop(0, seqs, regroup, 0, unroll=4)

    def each(g, body):
        for u in range(GROUP):
            body(g * GROUP + u)

    def wait_for(hbm, vmem, sem, g):
        part = pl.ds(g * GROUP, GROUP)
        pltpu.make_async_copy(hbm.at[pl.ds(0, GROUP)], vmem.at[part], sem.at[g]).wait()

    def score(i):
        s = seq_of(i)
        for j in range(pairs):
            keys = k_ref[i, 2 * j : 2 * j + 2].reshape(256, 128)
            both = lax.dot_general(
                q_ref[s, j], keys, (((1,), (1,)), ((), ())), preferred_element_type=jnp.float32
            )
            for h in range(2):
                rows = slice(8 * h, 8 * h + 8)
                score_ref[i, j, h] = jnp.where(upper, both[rows, :128], both[rows, 128:])

    def weigh(i):
        s = seq_of(i)
        inside = token < list_ref[i] // (pages * seqs)
        for j in range(pairs):
            for h in range(2):
                score = jnp.where(inside, score_ref[i, j, h], LOWEST)
                top = jnp.max(score, axis=1, keepdims=True)
                prob_ref[i, j, h] = jnp.where(inside, jnp.exp2((score - top) * scale2), 0.0)
                top = jnp.broadcast_to(top, (8, 128))
                pmax_ref[i, j, h] = top
                max_ref[s, j, h] = jnp.maximum(max_ref[s, j, h], top)

    def combine(i):
        for j in range(pairs):
            probs = jnp.concatenate([prob_ref[i, j, 0], prob_ref[i, j, 1]], axis=0)
            values = jnp.concatenate([v_ref[i, 2 * j], v_ref[i, 2 * j + 1]], axis=1)
            both = jnp.dot(probs.astype(jnp.bfloat16), values, preferred_element_type=jnp.float32)
            for h in range(2):
                rows = slice(8 * h, 8 * h + 8)
                score_ref[i, j, h] = jnp.where(upper, both[rows, :128], both[rows, 128:])

    def gather(i):
        s = seq_of(i)
        for j in range(pairs):
            for h in range(2):
                factor = jnp.exp2((pmax_ref[i, j, h] - max_ref[s, j, h]) * scale2)
                sum_ref[s, j, h] = sum_ref[s, j, h] + factor * prob_ref[i, j, h]
                out_ref[s, j, h] = out_ref[s, j, h] + factor * score_ref[i, j, h]

    def staged(hbm, vmem, sem, first, second):
        wait_for(hbm, vmem, sem, 0)
        each(0, first)

        def step(g, _):
            wait_for(hbm, vmem, sem, g)
            each(g - 1, second)
            each(g, first)
            return 0

        lax.fori_loop(1, groups, step, 0)
        each(groups - 1, second)

    staged(k_hbm, k_ref, k_sem, score, weigh)
    staged(v_hbm, v_ref, v_sem, combine, gather)

    kind = token & 3
    first = (token & 4) == 0
    block = lax.shift_right_logical(token, 3)

    def rounded(x):
        return x.astype(jnp.bfloat16).astype(jnp.float32)

    def pack(s, _):
        for h in range(2):
            to = (2 * s + h - RESULT_FIRST) & (2 * seqs - 1)
            note = jnp.zeros((8, 128), jnp.float32)
            powers = jnp.zeros((8, 128), jnp.float32)
            for j in range(pairs):
                out = out_ref[s, j, h]
                largest = jnp.max(jnp.abs(out), axis=1, keepdims=True)
                power = jnp.clip(jnp.ceil(-jnp.log2(largest)), 0.0, MOST_POWER)
                out = out * jnp.exp2(power)
                send_ref[to, 2 * j] = out[:4]
                send_ref[to, 2 * j + 1] = out[4:]
                total = jnp.sum(sum_ref[s, j, h], axis=1, keepdims=True)
                best = jnp.maximum(max_ref[s, j, h], NO_SCORE) * SCORE_UNIT
                note = jnp.where(kind == j, best, note)
                note = jnp.where(kind == pairs + j, total, note)
                powers = jnp.where(kind == j, power, powers)
            note = jnp.where(first, note, pltpu.roll(note, 4, 0))
            powers = jnp.where(first, powers, pltpu.roll(powers, 4, 0))
            high = rounded(note)
            middle = rounded(note - high)
            low = note - high - middle
            note = jnp.where(block == 0, high, jnp.where(block == 1, middle, low))
            send_ref[to, 2 * pairs] = jnp.where(block < 3, note, powers)[:4]
        return 0

    lax.fori_loop(0, seqs, pack, 0, unroll=4)


def attend(plan, arrived, key_cache, value_cache):
    pages_here, kv_here, page_len, head_width = key_cache.shape
    devices, rows, _ = arrived.shape
    seq_count, pairs = devices // 2, kv_here // 2
    scale2 = math.log2(math.e) / math.sqrt(head_width)
    vmem = pl.BlockSpec(memory_space=pltpu.VMEM)
    smem = pl.BlockSpec(memory_space=pltpu.SMEM)
    hbm = pl.BlockSpec(memory_space=pltpu.HBM)
    by_page = pltpu.VMEM((pages_here, pairs, 2, 8, 128), jnp.float32)
    by_seq = pltpu.VMEM((seq_count, pairs, 2, 8, 128), jnp.float32)
    cached = pltpu.VMEM(key_cache.shape, jnp.bfloat16)
    return pl.pallas_call(
        lambda *refs: attend_kernel(scale2, *refs),
        out_shape=jax.ShapeDtypeStruct((devices, kv_here + 1, rows // kv_here, head_width), jnp.float32),
        in_specs=[smem, vmem, hbm, hbm],
        out_specs=vmem,
        scratch_shapes=[
            pltpu.SMEM((pages_here + GROUP,), jnp.int32),
            cached,
            cached,
            pltpu.VMEM((seq_count, pairs, 16, head_width), jnp.bfloat16),
            by_page,
            by_page,
            by_page,
            by_seq,
            by_seq,
            by_seq,
            pltpu.SemaphoreType.DMA((pages_here // GROUP,)),
            pltpu.SemaphoreType.DMA((pages_here // GROUP,)),
        ],
        name="attend",
        compiler_params=pltpu.CompilerParams(vmem_limit_bytes=52 * MIB),
    )(plan, arrived, key_cache, value_cache)


def merge_kernel(scale2, recv_ref, q_ref, k_ref, v_ref, o_ref):
    heads, local_rows, width = q_ref.shape
    lines = recv_ref.shape[1]
    pairs = heads // 2
    own = lax.axis_index("kv") * k_ref.shape[0] // (lines // local_rows)
    unit = scale2 / SCORE_UNIT
    notes = recv_ref[heads].astype(jnp.bfloat16)
    row = lax.broadcasted_iota(jnp.int32, (width, width), 0)

    def column(at, chosen):
        return jnp.where(((row & 7) == at) & chosen, 1.0, 0.0).astype(jnp.bfloat16)

    def picked(first, second):
        wide = jnp.concatenate([first, second], axis=1)
        both = jnp.dot(notes, wide, preferred_element_type=jnp.float32)
        return both[:, :width], both[:, width:]

    def at(g):
        return (g % 2) * 4 + g // 2

    powers = []
    for g in range(0, heads, 2):
        powers += picked(*(column(at(g + u), (row >= 24) & (row < 32)) for u in range(2)))
    keys = k_ref[own].astype(jnp.float32)
    fresh = v_ref[own].astype(jnp.float32)

    def folded(x, join):
        return join(x, pltpu.roll(x, 4, 0))

    for g in range(heads):
        best, sums = picked(column(at(g), row < 24), column(at(g) + pairs, row < 24))
        query = q_ref[g].astype(jnp.float32)
        query = jnp.concatenate([query, query], axis=0)
        new = jnp.sum(query * keys[g : g + 1], axis=1, keepdims=True) * SCORE_UNIT
        top = best[:8]
        for k in range(8, lines, 8):
            top = jnp.maximum(top, best[k : k + 8])
        top = jnp.maximum(folded(top, jnp.maximum), new)
        weight = jnp.exp2((new - top) * unit)
        total = jnp.zeros((8, width), jnp.float32)
        out = jnp.zeros((8, width), jnp.float32)
        for k in range(0, lines, 8):
            exponent = (best[k : k + 8] - top) * unit
            total = total + jnp.exp2(exponent) * sums[k : k + 8]
            out = out + jnp.exp2(exponent - powers[g][k : k + 8]) * recv_ref[g, k : k + 8]
        total = folded(total, jnp.add) + weight
        out = folded(out, jnp.add) + weight * fresh[g : g + 1]
        o_ref[g] = (out / total)[:local_rows].astype(o_ref.dtype)


def plan_kernel(pages, page_len, table_ref, lengths_ref, plan_ref):
    seqs, slots = table_ref.shape
    row = lax.broadcasted_iota(jnp.int32, (seqs, slots), 0)
    slot = lax.broadcasted_iota(jnp.int32, (seqs, slots), 1)
    square = (seqs, seqs)
    same = lax.broadcasted_iota(jnp.int32, square, 0) == lax.broadcasted_iota(jnp.int32, square, 1)
    length = jnp.sum(
        jnp.where(same, lengths_ref[...].astype(jnp.float32), 0.0), axis=1, keepdims=True
    ).astype(jnp.int32)
    inside = jnp.clip(length - 1 - slot * page_len, 0, page_len)
    code = (row + seqs * inside).astype(jnp.float32)
    local = table_ref[...] - lax.axis_index("kv") * pages
    lane = lax.broadcasted_iota(jnp.int32, (8, 128), 1)
    found = jnp.zeros((8, 128), jnp.float32)
    for p in range(pages):
        hit = jnp.where(local == p, code, 0.0)
        hit = sum(hit[8 * i : 8 * i + 8] for i in range(seqs // 8))
        found = jnp.where(lane == p, jnp.sum(hit, axis=1, keepdims=True), found)
    plan_ref[...] = jnp.sum(found, axis=0, keepdims=True).astype(jnp.int32)


def plan_pages(pages, page_len, lengths, page_table):
    seqs = lengths.shape[0]
    slots = page_table.shape[0] // seqs
    vmem = pl.BlockSpec(memory_space=pltpu.VMEM)
    return pl.pallas_call(
        lambda *refs: plan_kernel(pages, page_len, *refs),
        out_shape=jax.ShapeDtypeStruct((1, 128), jnp.int32),
        in_specs=[vmem, vmem],
        out_specs=vmem,
        name="plan",
        cost_estimate=pl.CostEstimate(flops=10**9, bytes_accessed=10**5, transcendentals=0),
        compiler_params=pltpu.CompilerParams(vmem_limit_bytes=2 * MIB),
    )(page_table.reshape(seqs, slots), lengths.reshape(1, seqs))


def exchange(x, first):
    devices = x.shape[0]
    order = [(d + first) % devices for d in range(devices)]
    return lax.all_to_all(x, "kv", 0, 0, tiled=True, axis_index_groups=[order])


def on_device(queries, key_cache, value_cache, key_new, value_new, lengths, page_table):
    kv_here, local_rows, head_width = queries.shape
    pages_here = key_cache.shape[0]
    page_len = key_cache.shape[2]
    seq_count = lengths.shape[0]
    devices = lax.axis_size("kv")
    pairs = kv_here // 2
    rows = kv_here * local_rows
    scale2 = math.log2(math.e) / math.sqrt(head_width)
    kv_index = lax.axis_index("kv")

    mine = queries.reshape(rows, head_width)
    arrived = exchange(jnp.broadcast_to(mine[None], (devices, rows, head_width)), QUERY_FIRST)
    plan = plan_pages(pages_here, page_len, lengths, page_table)
    sent = attend(plan, arrived, key_cache, value_cache)

    vmem = pl.BlockSpec(memory_space=pltpu.VMEM)
    received = exchange(sent.astype(jnp.float16), RESULT_FIRST).astype(jnp.float32)
    received = jnp.transpose(received, (1, 0, 2, 3)).reshape(kv_here + 1, devices * local_rows, head_width)

    return pl.pallas_call(
        lambda *refs: merge_kernel(scale2, *refs),
        out_shape=jax.ShapeDtypeStruct(queries.shape, jnp.bfloat16),
        in_specs=[vmem] * 4,
        out_specs=vmem,
        name="merge",
        compiler_params=pltpu.CompilerParams(vmem_limit_bytes=8 * MIB),
    )(received, queries, key_new, value_new)


def solution(mesh):
    placed = (
        P("head", "kv", None),
        P("kv", "head", None, None),
        P("kv", "head", None, None),
        P(None, "head", None),
        P(None, "head", None),
        P(),
        P(),
    )
    return jax.shard_map(
        on_device, mesh=mesh, in_specs=placed, out_specs=P("head", "kv", None), check_vma=False
    )
```

```python
import math

import jax
import jax.numpy as jnp
from jax import lax
from jax.experimental import pallas as pl
from jax.experimental.pallas import tpu as pltpu
from jax.sharding import PartitionSpec as P

LOWEST = -1e30
SCORE_UNIT = 1.0 / 8.0
NO_SCORE = -480000.0
MOST_POWER = 120.0
GROUP = 8
FIRST = 42
MIB = 1024 * 1024


def attend_kernel(
    scale2, plan_ref, arrived_ref, k_hbm, v_hbm, send_ref,
    list_ref, k_ref, v_ref, q_ref, score_ref, prob_ref, pmax_ref, max_ref, sum_ref, out_ref, k_sem, v_sem,
):
    pages = k_ref.shape[0]
    seqs, pairs = q_ref.shape[0], q_ref.shape[1]
    page_bits, group_bits = pages.bit_length() - 1, GROUP.bit_length() - 1
    code_bits = page_bits + seqs.bit_length() - 1
    shift = lax.shift_right_logical
    token = lax.broadcasted_iota(jnp.int32, (8, 128), 1)
    upper = lax.broadcasted_iota(jnp.int32, (8, 128), 0) < 4

    def page_of(i):
        return list_ref[i] & (pages - 1)

    def seq_of(i):
        return shift(list_ref[i], page_bits) & (seqs - 1)

    def start(hbm, vmem, sem, i):
        pltpu.make_async_copy(hbm.at[page_of(i)], vmem.at[i], sem.at[shift(i, group_bits)]).start()

    def find(p, count):
        code = plan_ref[0, p]
        used = code >= seqs
        list_ref[count] = (code << page_bits) + p

        @pl.when(used)
        def _():
            start(k_hbm, k_ref, k_sem, count)

        return count + used.astype(jnp.int32)

    count = lax.fori_loop(0, pages, find, 0, unroll=4)
    groups = jnp.maximum(shift(count + GROUP - 1, group_bits), 1)

    def pad(i, _):
        list_ref[i] = 0
        start(k_hbm, k_ref, k_sem, i)
        return 0

    lax.fori_loop(count, groups * GROUP, pad, 0)

    def rest(g, _):
        for u in range(GROUP):
            start(v_hbm, v_ref, v_sem, g * GROUP + u)
        return 0

    lax.fori_loop(0, groups, rest, 0)

    max_ref[...] = jnp.full(max_ref.shape, LOWEST, jnp.float32)
    sum_ref[...] = jnp.zeros(sum_ref.shape, jnp.float32)
    out_ref[...] = jnp.zeros(out_ref.shape, jnp.float32)

    def regroup(s, _):
        for h in range(2):
            for j in range(pairs):
                q_ref[s, j, 8 * h : 8 * h + 8] = arrived_ref[(2 * s + h - FIRST) % (2 * seqs), 8 * j : 8 * j + 8]
        return 0

    for s in range(seqs):
        regroup(s, 0)

    def each(g, body):
        for u in range(GROUP):
            body(g * GROUP + u)

    def wait_for(hbm, vmem, sem, g):
        part = pl.ds(g * GROUP, GROUP)
        pltpu.make_async_copy(hbm.at[pl.ds(0, GROUP)], vmem.at[part], sem.at[g]).wait()

    def score(i):
        s = seq_of(i)
        for j in range(pairs):
            keys = k_ref[i, 2 * j : 2 * j + 2].reshape(256, 128)
            both = lax.dot_general(
                q_ref[s, j], keys, (((1,), (1,)), ((), ())), preferred_element_type=jnp.float32
            )
            for h in range(2):
                rows = slice(8 * h, 8 * h + 8)
                score_ref[i, j, h] = jnp.where(upper, both[rows, :128], both[rows, 128:])

    def weigh(i):
        s = seq_of(i)
        inside = token < shift(list_ref[i], code_bits)
        for j in range(pairs):
            for h in range(2):
                score = jnp.where(inside, score_ref[i, j, h], LOWEST)
                top = jnp.max(score, axis=1, keepdims=True)
                prob_ref[i, j, h] = jnp.where(inside, jnp.exp2((score - top) * scale2), 0.0)
                top = jnp.broadcast_to(top, (8, 128))
                pmax_ref[i, j, h] = top
                max_ref[s, j, h] = jnp.maximum(max_ref[s, j, h], top)

    def combine(i):
        for j in range(pairs):
            probs = jnp.concatenate([prob_ref[i, j, 0], prob_ref[i, j, 1]], axis=0)
            values = jnp.concatenate([v_ref[i, 2 * j], v_ref[i, 2 * j + 1]], axis=1)
            both = jnp.dot(probs.astype(jnp.bfloat16), values, preferred_element_type=jnp.float32)
            for h in range(2):
                rows = slice(8 * h, 8 * h + 8)
                score_ref[i, j, h] = jnp.where(upper, both[rows, :128], both[rows, 128:])

    def gather(i):
        s = seq_of(i)
        for j in range(pairs):
            for h in range(2):
                factor = jnp.exp2((pmax_ref[i, j, h] - max_ref[s, j, h]) * scale2)
                sum_ref[s, j, h] = sum_ref[s, j, h] + factor * prob_ref[i, j, h]
                out_ref[s, j, h] = out_ref[s, j, h] + factor * score_ref[i, j, h]

    def staged(hbm, vmem, sem, first, second):
        wait_for(hbm, vmem, sem, 0)
        each(0, first)

        def step(g, _):
            wait_for(hbm, vmem, sem, g)
            each(g - 1, second)
            each(g, first)
            return 0

        lax.fori_loop(1, groups, step, 0)
        each(groups - 1, second)

    staged(k_hbm, k_ref, k_sem, score, weigh)
    staged(v_hbm, v_ref, v_sem, combine, gather)

    kind = token & 3
    first = (token & 4) == 0
    block = lax.shift_right_logical(token, 3)
    is_score = kind < pairs

    def rounded(x):
        return x.astype(jnp.bfloat16).astype(jnp.float32)

    def halves(one, two):
        low = jnp.where(upper, one, pltpu.roll(two, 4, 0))
        high = jnp.where(upper, pltpu.roll(one, 4, 0), two)
        return jnp.where(first, low, high)

    def pack(s, _):
        places = [(2 * s + h - FIRST) % (2 * seqs) for h in range(2)]
        outs = [[out_ref[s, j, h] for j in range(pairs)] for h in range(2)]
        largest = jnp.abs(outs[0][0])
        for out in outs[0][1:] + outs[1]:
            largest = jnp.maximum(largest, jnp.abs(out))
        largest = jnp.max(largest, axis=1, keepdims=True)
        power = jnp.clip(jnp.ceil(-jnp.log2(largest)), 0.0, MOST_POWER)
        power = jnp.broadcast_to(power, (8, 128))
        factor = jnp.exp2(power)
        notes = []
        for h in range(2):
            note = max_ref[s, 0, h]
            for j in range(1, pairs):
                note = jnp.where(kind == j, max_ref[s, j, h], note)
            for j in range(pairs):
                out = outs[h][j] * factor
                send_ref[places[h], 2 * j] = out[:4]
                send_ref[places[h], 2 * j + 1] = out[4:]
                total = jnp.sum(sum_ref[s, j, h], axis=1, keepdims=True)
                note = jnp.where(kind == pairs + j, total, note)
            notes.append(note)
        note = halves(*notes)
        note = jnp.where(is_score, jnp.maximum(note, NO_SCORE) * SCORE_UNIT, note)
        high = rounded(note)
        rest = note - high
        middle = rounded(rest)
        note = jnp.where(block == 0, high, jnp.where(block == 1, middle, rest - middle))
        note = jnp.where(block < 3, note, halves(power, power))
        send_ref[places[0], 2 * pairs] = note[:4]
        send_ref[places[1], 2 * pairs] = note[4:]
        return 0

    for s in range(seqs):
        pack(s, 0)


def attend(plan, arrived, key_cache, value_cache):
    pages_here, kv_here, page_len, head_width = key_cache.shape
    devices, rows, _ = arrived.shape
    seq_count, pairs = devices // 2, kv_here // 2
    scale2 = math.log2(math.e) / math.sqrt(head_width)
    vmem = pl.BlockSpec(memory_space=pltpu.VMEM)
    smem = pl.BlockSpec(memory_space=pltpu.SMEM)
    hbm = pl.BlockSpec(memory_space=pltpu.HBM)
    by_page = pltpu.VMEM((pages_here, pairs, 2, 8, 128), jnp.float32)
    by_seq = pltpu.VMEM((seq_count, pairs, 2, 8, 128), jnp.float32)
    cached = pltpu.VMEM(key_cache.shape, jnp.bfloat16)
    return pl.pallas_call(
        lambda *refs: attend_kernel(scale2, *refs),
        out_shape=jax.ShapeDtypeStruct((devices, kv_here + 1, rows // kv_here, head_width), jnp.float32),
        in_specs=[smem, vmem, hbm, hbm],
        out_specs=vmem,
        scratch_shapes=[
            pltpu.SMEM((pages_here + GROUP,), jnp.int32),
            cached,
            cached,
            pltpu.VMEM((seq_count, pairs, 16, head_width), jnp.bfloat16),
            by_page,
            by_page,
            by_page,
            by_seq,
            by_seq,
            by_seq,
            pltpu.SemaphoreType.DMA((pages_here // GROUP,)),
            pltpu.SemaphoreType.DMA((pages_here // GROUP,)),
        ],
        name="attend",
        compiler_params=pltpu.CompilerParams(vmem_limit_bytes=52 * MIB),
    )(plan, arrived, key_cache, value_cache)


def merge_kernel(scale2, recv_ref, q_ref, k_ref, v_ref, o_ref):
    heads, local_rows, width = q_ref.shape
    lines = recv_ref.shape[1]
    pairs = heads // 2
    own = lax.axis_index("kv") * k_ref.shape[0] // (lines // local_rows)
    unit = scale2 / SCORE_UNIT
    notes = recv_ref[heads].astype(jnp.bfloat16)
    row = lax.broadcasted_iota(jnp.int32, (width, width), 0)

    def column(at, chosen):
        return jnp.where(((row & 7) == at) & chosen, 1.0, 0.0).astype(jnp.bfloat16)

    def picked(first, second):
        wide = jnp.concatenate([first, second], axis=1)
        both = jnp.dot(notes, wide, preferred_element_type=jnp.float32)
        return both[:, :width], both[:, width:]

    def at(g):
        return (g % 2) * 4 + g // 2

    powers = []
    for g in range(0, heads, 2):
        powers += picked(*(column(at(g + u), (row >= 24) & (row < 32)) for u in range(2)))
    keys = k_ref[own].astype(jnp.float32)
    fresh = v_ref[own].astype(jnp.float32)

    def folded(x, join):
        return join(x, pltpu.roll(x, 4, 0))

    for g in range(heads):
        best, sums = picked(column(at(g), row < 24), column(at(g) + pairs, row < 24))
        query = q_ref[g].astype(jnp.float32)
        query = jnp.concatenate([query, query], axis=0)
        new = jnp.sum(query * keys[g : g + 1], axis=1, keepdims=True) * SCORE_UNIT
        top = best[:8]
        for k in range(8, lines, 8):
            top = jnp.maximum(top, best[k : k + 8])
        top = jnp.maximum(folded(top, jnp.maximum), new)
        weight = jnp.exp2((new - top) * unit)
        total = jnp.zeros((8, width), jnp.float32)
        out = jnp.zeros((8, width), jnp.float32)
        for k in range(0, lines, 8):
            exponent = (best[k : k + 8] - top) * unit
            total = total + jnp.exp2(exponent) * sums[k : k + 8]
            out = out + jnp.exp2(exponent - powers[g][k : k + 8]) * recv_ref[g, k : k + 8]
        total = folded(total, jnp.add) + weight
        out = folded(out, jnp.add) + weight * fresh[g : g + 1]
        o_ref[g] = (out / total)[:local_rows].astype(o_ref.dtype)


def plan_kernel(pages, page_len, table_ref, lengths_ref, plan_ref):
    seqs, slots = table_ref.shape
    row = lax.broadcasted_iota(jnp.int32, (seqs, slots), 0)
    slot = lax.broadcasted_iota(jnp.int32, (seqs, slots), 1)
    square = (seqs, seqs)
    same = lax.broadcasted_iota(jnp.int32, square, 0) == lax.broadcasted_iota(jnp.int32, square, 1)
    length = jnp.sum(
        jnp.where(same, lengths_ref[...].astype(jnp.float32), 0.0), axis=1, keepdims=True
    ).astype(jnp.int32)
    inside = jnp.clip(length - 1 - slot * page_len, 0, page_len)
    code = (row + seqs * inside).astype(jnp.float32)
    local = table_ref[...] - lax.axis_index("kv") * pages
    lane = lax.broadcasted_iota(jnp.int32, (8, 128), 1)
    found = jnp.zeros((8, 128), jnp.float32)
    for p in range(pages):
        hit = jnp.where(local == p, code, 0.0)
        hit = sum(hit[8 * i : 8 * i + 8] for i in range(seqs // 8))
        found = jnp.where(lane == p, jnp.sum(hit, axis=1, keepdims=True), found)
    plan_ref[...] = jnp.sum(found, axis=0, keepdims=True).astype(jnp.int32)


def plan_pages(pages, page_len, lengths, page_table):
    seqs = lengths.shape[0]
    slots = page_table.shape[0] // seqs
    vmem = pl.BlockSpec(memory_space=pltpu.VMEM)
    return pl.pallas_call(
        lambda *refs: plan_kernel(pages, page_len, *refs),
        out_shape=jax.ShapeDtypeStruct((1, 128), jnp.int32),
        in_specs=[vmem, vmem],
        out_specs=vmem,
        name="plan",
        cost_estimate=pl.CostEstimate(flops=10**9, bytes_accessed=10**5, transcendentals=0),
        compiler_params=pltpu.CompilerParams(vmem_limit_bytes=2 * MIB),
    )(page_table.reshape(seqs, slots), lengths.reshape(1, seqs))


def exchange(x):
    devices = x.shape[0]
    order = [(d + FIRST) % devices for d in range(devices)]
    return lax.all_to_all(x, "kv", 0, 0, tiled=True, axis_index_groups=[order])


def on_device(queries, key_cache, value_cache, key_new, value_new, lengths, page_table):
    kv_here, local_rows, head_width = queries.shape
    pages_here = key_cache.shape[0]
    page_len = key_cache.shape[2]
    seq_count = lengths.shape[0]
    devices = lax.axis_size("kv")
    pairs = kv_here // 2
    rows = kv_here * local_rows
    scale2 = math.log2(math.e) / math.sqrt(head_width)
    kv_index = lax.axis_index("kv")

    mine = queries.reshape(rows, head_width)
    arrived = exchange(jnp.broadcast_to(mine[None], (devices, rows, head_width)))
    plan = plan_pages(pages_here, page_len, lengths, page_table)
    sent = attend(plan, arrived, key_cache, value_cache)

    vmem = pl.BlockSpec(memory_space=pltpu.VMEM)
    received = exchange(sent.astype(jnp.float16)).astype(jnp.float32)
    received = jnp.transpose(received, (1, 0, 2, 3)).reshape(kv_here + 1, devices * local_rows, head_width)

    return pl.pallas_call(
        lambda *refs: merge_kernel(scale2, *refs),
        out_shape=jax.ShapeDtypeStruct(queries.shape, jnp.bfloat16),
        in_specs=[vmem] * 4,
        out_specs=vmem,
        name="merge",
        compiler_params=pltpu.CompilerParams(vmem_limit_bytes=8 * MIB),
    )(received, queries, key_new, value_new)


def solution(mesh):
    placed = (
        P("head", "kv", None),
        P("kv", "head", None, None),
        P("kv", "head", None, None),
        P(None, "head", None),
        P(None, "head", None),
        P(),
        P(),
    )
    return jax.shard_map(
        on_device, mesh=mesh, in_specs=placed, out_specs=P("head", "kv", None), check_vma=False
    )
```

```python
import math

import jax
import jax.numpy as jnp
from jax import lax
from jax.experimental import pallas as pl
from jax.experimental.pallas import tpu as pltpu
from jax.sharding import PartitionSpec as P

LOWEST = -1e30
SCORE_UNIT = 1.0 / 8.0
NO_SCORE = -480000.0
MOST_POWER = 120.0
GROUP = 8
FIRST = 42
MIB = 1024 * 1024


def attend_kernel(
    scale2, plan_ref, arrived_ref, k_hbm, v_hbm, send_ref,
    list_ref, k_ref, v_ref, q_ref, score_ref, prob_ref, pmax_ref, max_ref, sum_ref, out_ref, k_sem, v_sem,
):
    pages = k_ref.shape[0]
    seqs, pairs = q_ref.shape[0], q_ref.shape[1]
    page_bits, group_bits = pages.bit_length() - 1, GROUP.bit_length() - 1
    code_bits = page_bits + seqs.bit_length() - 1
    shift = lax.shift_right_logical
    token = lax.broadcasted_iota(jnp.int32, (8, 128), 1)
    upper = lax.broadcasted_iota(jnp.int32, (8, 128), 0) < 4

    def page_of(i):
        return list_ref[i] & (pages - 1)

    def seq_of(i):
        return shift(list_ref[i], page_bits) & (seqs - 1)

    def start(hbm, vmem, sem, i, priority=0):
        pltpu.make_async_copy(hbm.at[page_of(i)], vmem.at[i], sem.at[shift(i, group_bits)]).start(priority=priority)

    def find(p, count):
        code = plan_ref[0, p]
        used = code >= seqs
        list_ref[count] = (code << page_bits) + p

        @pl.when(used)
        def _():
            start(k_hbm, k_ref, k_sem, count)

        return count + used.astype(jnp.int32)

    count = lax.fori_loop(0, pages, find, 0, unroll=4)
    groups = jnp.maximum(shift(count + GROUP - 1, group_bits), 1)

    def pad(i, _):
        list_ref[i] = 0
        start(k_hbm, k_ref, k_sem, i)
        return 0

    lax.fori_loop(count, groups * GROUP, pad, 0)

    def rest(g, _):
        for u in range(GROUP):
            start(v_hbm, v_ref, v_sem, g * GROUP + u, priority=1)
        return 0

    lax.fori_loop(0, groups, rest, 0)

    max_ref[...] = jnp.full(max_ref.shape, LOWEST, jnp.float32)
    sum_ref[...] = jnp.zeros(sum_ref.shape, jnp.float32)
    out_ref[...] = jnp.zeros(out_ref.shape, jnp.float32)

    def regroup(s, _):
        for h in range(2):
            for j in range(pairs):
                q_ref[s, j, 8 * h : 8 * h + 8] = arrived_ref[(2 * s + h - FIRST) % (2 * seqs), 8 * j : 8 * j + 8]
        return 0

    for s in range(seqs):
        regroup(s, 0)

    def each(g, body):
        for u in range(GROUP):
            body(g * GROUP + u)

    def wait_for(hbm, vmem, sem, g):
        part = pl.ds(g * GROUP, GROUP)
        pltpu.make_async_copy(hbm.at[pl.ds(0, GROUP)], vmem.at[part], sem.at[g]).wait()

    def score(i):
        s = seq_of(i)
        for j in range(pairs):
            keys = k_ref[i, 2 * j : 2 * j + 2].reshape(256, 128)
            both = lax.dot_general(
                q_ref[s, j], keys, (((1,), (1,)), ((), ())), preferred_element_type=jnp.float32
            )
            for h in range(2):
                rows = slice(8 * h, 8 * h + 8)
                score_ref[i, j, h] = jnp.where(upper, both[rows, :128], both[rows, 128:])

    def weigh(i):
        s = seq_of(i)
        inside = token < shift(list_ref[i], code_bits)
        for j in range(pairs):
            for h in range(2):
                score = jnp.where(inside, score_ref[i, j, h], LOWEST)
                top = jnp.max(score, axis=1, keepdims=True)
                prob_ref[i, j, h] = jnp.where(inside, jnp.exp2((score - top) * scale2), 0.0)
                top = jnp.broadcast_to(top, (8, 128))
                pmax_ref[i, j, h] = top
                max_ref[s, j, h] = jnp.maximum(max_ref[s, j, h], top)

    def combine(i):
        for j in range(pairs):
            probs = jnp.concatenate([prob_ref[i, j, 0], prob_ref[i, j, 1]], axis=0)
            values = jnp.concatenate([v_ref[i, 2 * j], v_ref[i, 2 * j + 1]], axis=1)
            both = jnp.dot(probs.astype(jnp.bfloat16), values, preferred_element_type=jnp.float32)
            for h in range(2):
                rows = slice(8 * h, 8 * h + 8)
                score_ref[i, j, h] = jnp.where(upper, both[rows, :128], both[rows, 128:])

    def gather(i):
        s = seq_of(i)
        for j in range(pairs):
            for h in range(2):
                factor = jnp.exp2((pmax_ref[i, j, h] - max_ref[s, j, h]) * scale2)
                sum_ref[s, j, h] = sum_ref[s, j, h] + factor * prob_ref[i, j, h]
                out_ref[s, j, h] = out_ref[s, j, h] + factor * score_ref[i, j, h]

    def staged(hbm, vmem, sem, first, second):
        wait_for(hbm, vmem, sem, 0)
        each(0, first)

        def step(g, _):
            wait_for(hbm, vmem, sem, g)
            each(g - 1, second)
            each(g, first)
            return 0

        lax.fori_loop(1, groups, step, 0)
        each(groups - 1, second)

    staged(k_hbm, k_ref, k_sem, score, weigh)
    staged(v_hbm, v_ref, v_sem, combine, gather)

    kind = token & 3
    first = (token & 4) == 0
    block = lax.shift_right_logical(token, 3)
    is_score = kind < pairs

    def rounded(x):
        return x.astype(jnp.bfloat16).astype(jnp.float32)

    def halves(one, two):
        low = jnp.where(upper, one, pltpu.roll(two, 4, 0))
        high = jnp.where(upper, pltpu.roll(one, 4, 0), two)
        return jnp.where(first, low, high)

    def pack(s, _):
        places = [(2 * s + h - FIRST) % (2 * seqs) for h in range(2)]
        outs = [[out_ref[s, j, h] for j in range(pairs)] for h in range(2)]
        largest = jnp.abs(outs[0][0])
        for out in outs[0][1:] + outs[1]:
            largest = jnp.maximum(largest, jnp.abs(out))
        largest = jnp.max(largest, axis=1, keepdims=True)
        power = jnp.clip(jnp.ceil(-jnp.log2(largest)), 0.0, MOST_POWER)
        power = jnp.broadcast_to(power, (8, 128))
        factor = jnp.exp2(power)
        notes = []
        for h in range(2):
            note = max_ref[s, 0, h]
            for j in range(1, pairs):
                note = jnp.where(kind == j, max_ref[s, j, h], note)
            for j in range(pairs):
                out = outs[h][j] * factor
                send_ref[places[h], 2 * j] = out[:4]
                send_ref[places[h], 2 * j + 1] = out[4:]
                total = jnp.sum(sum_ref[s, j, h], axis=1, keepdims=True)
                note = jnp.where(kind == pairs + j, total, note)
            notes.append(note)
        note = halves(*notes)
        note = jnp.where(is_score, jnp.maximum(note, NO_SCORE) * SCORE_UNIT, note)
        high = rounded(note)
        rest = note - high
        middle = rounded(rest)
        note = jnp.where(block == 0, high, jnp.where(block == 1, middle, rest - middle))
        note = jnp.where(block < 3, note, halves(power, power))
        send_ref[places[0], 2 * pairs] = note[:4]
        send_ref[places[1], 2 * pairs] = note[4:]
        return 0

    for s in range(seqs):
        pack(s, 0)


def attend(plan, arrived, key_cache, value_cache):
    pages_here, kv_here, page_len, head_width = key_cache.shape
    devices, rows, _ = arrived.shape
    seq_count, pairs = devices // 2, kv_here // 2
    scale2 = math.log2(math.e) / math.sqrt(head_width)
    vmem = pl.BlockSpec(memory_space=pltpu.VMEM)
    smem = pl.BlockSpec(memory_space=pltpu.SMEM)
    hbm = pl.BlockSpec(memory_space=pltpu.HBM)
    by_page = pltpu.VMEM((pages_here, pairs, 2, 8, 128), jnp.float32)
    by_seq = pltpu.VMEM((seq_count, pairs, 2, 8, 128), jnp.float32)
    cached = pltpu.VMEM(key_cache.shape, jnp.bfloat16)
    return pl.pallas_call(
        lambda *refs: attend_kernel(scale2, *refs),
        out_shape=jax.ShapeDtypeStruct((devices, kv_here + 1, rows // kv_here, head_width), jnp.float32),
        in_specs=[smem, vmem, hbm, hbm],
        out_specs=vmem,
        scratch_shapes=[
            pltpu.SMEM((pages_here + GROUP,), jnp.int32),
            cached,
            cached,
            pltpu.VMEM((seq_count, pairs, 16, head_width), jnp.bfloat16),
            by_page,
            by_page,
            by_page,
            by_seq,
            by_seq,
            by_seq,
            pltpu.SemaphoreType.DMA((pages_here // GROUP,)),
            pltpu.SemaphoreType.DMA((pages_here // GROUP,)),
        ],
        name="attend",
        compiler_params=pltpu.CompilerParams(vmem_limit_bytes=52 * MIB),
    )(plan, arrived, key_cache, value_cache)


def merge_kernel(scale2, recv_ref, q_ref, k_ref, v_ref, o_ref):
    heads, local_rows, width = q_ref.shape
    lines = recv_ref.shape[1]
    pairs = heads // 2
    own = lax.axis_index("kv") * k_ref.shape[0] // (lines // local_rows)
    unit = scale2 / SCORE_UNIT
    notes = recv_ref[heads].astype(jnp.bfloat16)
    row = lax.broadcasted_iota(jnp.int32, (width, width), 0)

    def column(at, chosen):
        return jnp.where(((row & 7) == at) & chosen, 1.0, 0.0).astype(jnp.bfloat16)

    def picked(first, second):
        wide = jnp.concatenate([first, second], axis=1)
        both = jnp.dot(notes, wide, preferred_element_type=jnp.float32)
        return both[:, :width], both[:, width:]

    def at(g):
        return (g % 2) * 4 + g // 2

    powers = []
    for g in range(0, heads, 2):
        powers += picked(*(column(at(g + u), (row >= 24) & (row < 32)) for u in range(2)))
    keys = k_ref[own].astype(jnp.float32)
    fresh = v_ref[own].astype(jnp.float32)

    def folded(x, join):
        return join(x, pltpu.roll(x, 4, 0))

    for g in range(heads):
        best, sums = picked(column(at(g), row < 24), column(at(g) + pairs, row < 24))
        query = q_ref[g].astype(jnp.float32)
        query = jnp.concatenate([query, query], axis=0)
        new = jnp.sum(query * keys[g : g + 1], axis=1, keepdims=True) * SCORE_UNIT
        top = best[:8]
        for k in range(8, lines, 8):
            top = jnp.maximum(top, best[k : k + 8])
        top = jnp.maximum(folded(top, jnp.maximum), new)
        weight = jnp.exp2((new - top) * unit)
        total = jnp.zeros((8, width), jnp.float32)
        out = jnp.zeros((8, width), jnp.float32)
        for k in range(0, lines, 8):
            exponent = (best[k : k + 8] - top) * unit
            total = total + jnp.exp2(exponent) * sums[k : k + 8]
            out = out + jnp.exp2(exponent - powers[g][k : k + 8]) * recv_ref[g, k : k + 8]
        total = folded(total, jnp.add) + weight
        out = folded(out, jnp.add) + weight * fresh[g : g + 1]
        o_ref[g] = (out / total)[:local_rows].astype(o_ref.dtype)


def plan_kernel(pages, page_len, table_ref, lengths_ref, plan_ref):
    seqs, slots = table_ref.shape
    row = lax.broadcasted_iota(jnp.int32, (seqs, slots), 0)
    slot = lax.broadcasted_iota(jnp.int32, (seqs, slots), 1)
    square = (seqs, seqs)
    same = lax.broadcasted_iota(jnp.int32, square, 0) == lax.broadcasted_iota(jnp.int32, square, 1)
    length = jnp.sum(
        jnp.where(same, lengths_ref[...].astype(jnp.float32), 0.0), axis=1, keepdims=True
    ).astype(jnp.int32)
    inside = jnp.clip(length - 1 - slot * page_len, 0, page_len)
    code = (row + seqs * inside).astype(jnp.float32)
    local = table_ref[...] - lax.axis_index("kv") * pages
    lane = lax.broadcasted_iota(jnp.int32, (8, 128), 1)
    found = jnp.zeros((8, 128), jnp.float32)
    for p in range(pages):
        hit = jnp.where(local == p, code, 0.0)
        hit = sum(hit[8 * i : 8 * i + 8] for i in range(seqs // 8))
        found = jnp.where(lane == p, jnp.sum(hit, axis=1, keepdims=True), found)
    plan_ref[...] = jnp.sum(found, axis=0, keepdims=True).astype(jnp.int32)


def plan_pages(pages, page_len, lengths, page_table):
    seqs = lengths.shape[0]
    slots = page_table.shape[0] // seqs
    vmem = pl.BlockSpec(memory_space=pltpu.VMEM)
    return pl.pallas_call(
        lambda *refs: plan_kernel(pages, page_len, *refs),
        out_shape=jax.ShapeDtypeStruct((1, 128), jnp.int32),
        in_specs=[vmem, vmem],
        out_specs=vmem,
        name="plan",
        cost_estimate=pl.CostEstimate(flops=10**9, bytes_accessed=10**5, transcendentals=0),
        compiler_params=pltpu.CompilerParams(vmem_limit_bytes=2 * MIB),
    )(page_table.reshape(seqs, slots), lengths.reshape(1, seqs))


def exchange(x):
    devices = x.shape[0]
    order = [(d + FIRST) % devices for d in range(devices)]
    return lax.all_to_all(x, "kv", 0, 0, tiled=True, axis_index_groups=[order])


def on_device(queries, key_cache, value_cache, key_new, value_new, lengths, page_table):
    kv_here, local_rows, head_width = queries.shape
    pages_here = key_cache.shape[0]
    page_len = key_cache.shape[2]
    seq_count = lengths.shape[0]
    devices = lax.axis_size("kv")
    pairs = kv_here // 2
    rows = kv_here * local_rows
    scale2 = math.log2(math.e) / math.sqrt(head_width)
    kv_index = lax.axis_index("kv")

    mine = queries.reshape(rows, head_width)
    arrived = exchange(jnp.broadcast_to(mine[None], (devices, rows, head_width)))
    plan = plan_pages(pages_here, page_len, lengths, page_table)
    sent = attend(plan, arrived, key_cache, value_cache)

    vmem = pl.BlockSpec(memory_space=pltpu.VMEM)
    received = exchange(sent.astype(jnp.float16)).astype(jnp.float32)
    received = jnp.transpose(received, (1, 0, 2, 3)).reshape(kv_here + 1, devices * local_rows, head_width)

    return pl.pallas_call(
        lambda *refs: merge_kernel(scale2, *refs),
        out_shape=jax.ShapeDtypeStruct(queries.shape, jnp.bfloat16),
        in_specs=[vmem] * 4,
        out_specs=vmem,
        name="merge",
        compiler_params=pltpu.CompilerParams(vmem_limit_bytes=8 * MIB),
    )(received, queries, key_new, value_new)


def solution(mesh):
    placed = (
        P("head", "kv", None),
        P("kv", "head", None, None),
        P("kv", "head", None, None),
        P(None, "head", None),
        P(None, "head", None),
        P(),
        P(),
    )
    return jax.shard_map(
        on_device, mesh=mesh, in_specs=placed, out_specs=P("head", "kv", None), check_vma=False
    )
```
